32 devices in a mesh: pipe: 4 (over x, core), expert: 4 (over z), tensor: 2 (over y).
Axes of the slice: x: 2, y: 2, z: 4, core: 2. Of those that a mesh axis runs over, the one named last changes fastest.
Arguments:
- stream: bfloat16 [2, 4, 64, 7168], P(None, 'pipe', 'expert', 'tensor'), may hold values from -6 to 6
- expert_ids: int32 [2, 4, 64, 2], P(None, 'pipe', 'expert'), may hold values from 0 to 3, all different within a row; in each aligned block of 16 rows (0 to 15, 16 to 31, ..., all dimensions but the last counted through in order) at most 12 rows name the same one
- norm_gain: float32 [4, 7168], P('pipe', 'tensor'), may hold values from 0.1 to 1.9
- router: float32 [4, 7168, 4], P('pipe', 'tensor'), may hold values from -0.0625 to 0.0625
- w_up: bfloat16 [4, 7168, 1024], P('expert', 'tensor'), may hold values from -0.0625 to 0.0625
- w_down: bfloat16 [4, 1024, 7168], P('expert', None, 'tensor'), may hold values from -0.1875 to 0.1875
Outputs:
- result: bfloat16 [2, 4, 64, 7168], P(None, 'pipe', 'expert', 'tensor')
The draws below stay inside these ranges and needn't reach their ends.
Inputs may be any that keep to these rules, and one draw needn't show every extreme that they name: `expert_ids`: each token names 2 different experts. Among the 16 tokens of one direction held by one index of the expert axis at one section, at most 12 name any one expert, and in every draw some expert is named by exactly 12 of them.
All inputs are finite; a program needn't handle non-finite values.
Results may differ from the reference program's by a relative error of at most 0.0065.
Values may be sent and summed in bfloat16 or wider, within the bound.
No kernel may reach another device: no remote copies, remote signals or barrier semaphores. Data moves between devices by JAX's collectives and lax.ppermute only.
A program may use at most 64 MiB of HBM per device.

```python
import math
import jax
import jax.numpy as jnp
import numpy as np
from jax import lax

D = 7168
FF = 1024
TOK_DEV = 16
PIPE = 4
EXPERTS = 4
TOP = 2
TOKENS = 64
CAP = 12
N_EXPERT = 4


def shard_levels(stream_key, extent, split, smallest, top_value):
    factor_of, own = 1.0, jax.random.fold_in(stream_key, 6)
    for position, blocks in split:
        draws = jnp.exp(jax.random.uniform(jax.random.fold_in(own, position), (blocks,), jnp.float32, smallest / len(split), top_value / len(split)))
        factor_of = factor_of * jnp.repeat(draws, extent[position] // blocks).reshape([-1 if axis == position else 1 for axis in range(len(extent))])
    return factor_of


def shared_out(own_key, own, number, rows, count, top, bound, skew):
    order = jax.random.permutation(own_key, count)
    heavy_load, usual = shares(count, rows * top, bound, skew, True), shares(count, rows * top, bound, skew, False)
    places = jnp.arange(count)

    def named(lengths, rotation):
        used = int((lengths > 0).sum())
        fixed = max(1, used // 4)
        moved = fixed + (places - fixed + rotation * (used - fixed)) % max(1, count - fixed)
        return jnp.zeros((count,), jnp.int32).at[order[jnp.where(places < fixed, places, moved)]].set(jnp.asarray(lengths, jnp.int32))

    lengths = jnp.where(number % 4 == 0, named(heavy_load, number // 4), named(usual, number - number // 4 - 1))
    mixed = jax.random.permutation(jax.random.fold_in(own, 3), count)
    source_of, sink = mixed[0:count // 2 * 2:2], mixed[1:count // 2 * 2:2]
    slack = jnp.minimum(lengths[source_of] - 1, bound - lengths[sink]) // 2
    slack = jnp.where((source_of == order[0]) | (sink == order[0]) | (lengths[sink] == 0), 0, jnp.maximum(slack, 0))
    moved = jax.random.randint(jax.random.fold_in(own, 4), (count // 2,), 0, 1 << 20) % (slack + 1)
    lengths = lengths.at[source_of].add(-moved).at[sink].add(moved)
    items = jnp.searchsorted(jnp.cumsum(lengths), jnp.arange(rows * top), side="right").astype(jnp.int32)
    listing = items.reshape(top, rows).T
    listing = listing[jax.random.permutation(jax.random.fold_in(own, 1), rows)]
    rotation = jax.random.randint(jax.random.fold_in(own, 2), (rows, 1), 0, top)
    return jnp.take_along_axis(listing, (jnp.arange(top)[None, :] + rotation) % top, axis=1)


def shares(count, total, limit, lean, full):
    portions = [(1 << 20) // math.isqrt(grade ** lean) + 1 for grade in range(1, count + 1)]
    largest = limit if full else min(limit, max(-(-total // count), total * portions[0] // sum(portions)))
    least = 1 if total - largest >= count - 1 else 0
    counts, rest = [largest] + [least] * (count - 1), total - largest - least * (count - 1)
    while rest > 0:
        free = [i for i in range(1, count) if counts[i] < largest] or [i for i in range(1, count) if counts[i] < limit]
        mass, budget = sum([portions[i] for i in free]), rest
        for i in free:
            addition = min(limit - counts[i], max(1, budget * portions[i] // mass), rest)
            counts[i] = counts[i] + addition
            rest = rest - addition
    return np.array(counts)


def scatter_about(own_key, extent, scale, most, split=(), held_as=jnp.bfloat16):
    loudness = shard_levels(own_key, extent, split, -0.22, 0.18) if split else 1.0
    values = jax.random.normal(own_key, extent, jnp.float32) * scale * loudness
    return jnp.minimum(jnp.maximum(values, -most), most).astype(held_as)


def setup_inputs(seed: int = 0) -> dict:
    splits = jax.random.split(jax.random.key(seed), 7)
    stream = scatter_about(splits[0], (2, PIPE, TOKENS, D), 1.0, 6.0, ((1, 4), (2, 4), (3, 2)))
    expert_ids_keys = jax.random.split(jax.random.fold_in(splits[1], 1), 2 * PIPE * TOKENS // TOK_DEV)
    expert_ids_turns = jax.random.permutation(jax.random.fold_in(splits[1], 3), 2 * PIPE * TOKENS // TOK_DEV)
    expert_ids = jax.vmap(lambda own, number: shared_out(jax.random.fold_in(splits[1], 2), own, number, TOK_DEV, EXPERTS, TOP, CAP, 2))(expert_ids_keys, expert_ids_turns).reshape((2, PIPE, TOKENS, TOP))
    norm_gain = jnp.clip(1.0 + 0.18 * jax.random.normal(splits[2], (PIPE, D), jnp.float32), 0.1, 1.9)
    router = scatter_about(splits[3], (PIPE, D, EXPERTS), D ** -0.5, 0.0625, ((0, 4), (1, 2)), jnp.float32)
    w_up = scatter_about(splits[4], (EXPERTS, D, FF), D ** -0.5, 0.0625, ((0, 4), (1, 2)))
    w_down = scatter_about(splits[5], (EXPERTS, FF, D), FF ** -0.5, 0.1875, ((0, 4), (2, 2)))
    return dict(stream=stream, expert_ids=expert_ids, norm_gain=norm_gain, router=router, w_up=w_up, w_down=w_down)


norm_eps = 1e-06
route_scale = 2.5

def reference(stream, expert_ids, norm_gain, router, w_up, w_down):
    ahead = jnp.roll(stream[0], 1, axis=0)
    behind = jnp.roll(stream[1], -1, axis=0)
    arrived = jnp.stack([ahead, behind]).astype(jnp.float32)
    inverse = lax.rsqrt(lax.optimization_barrier(jnp.mean(arrived * arrived, axis=-1)) + norm_eps)
    normed = arrived * norm_gain[None, :, None, :] * inverse[..., None]
    logits = jnp.einsum('dptc,pce->dpte', normed, router, precision=lax.Precision.HIGHEST)
    picked = jnp.take_along_axis(logits, expert_ids, axis=-1)
    scores = jax.nn.sigmoid(picked)
    gates = route_scale * scores / lax.optimization_barrier(jnp.sum(scores, axis=-1, keepdims=True))
    hidden = normed.astype(jnp.bfloat16)
    groups = expert_ids.reshape(2, PIPE, N_EXPERT, TOK_DEV * TOP)
    onehot = (groups[..., None] == jnp.arange(EXPERTS, dtype=jnp.int32)).astype(jnp.int32)
    earlier = jnp.cumsum(onehot, axis=3) - onehot
    within = lax.optimization_barrier(jnp.sum(earlier * onehot, axis=-1))
    heading = lax.broadcasted_iota(jnp.int32, groups.shape, 0)
    section = lax.broadcasted_iota(jnp.int32, groups.shape, 1)
    member = lax.broadcasted_iota(jnp.int32, groups.shape, 2)
    entry = lax.broadcasted_iota(jnp.int32, groups.shape, 3)
    place = ((section * N_EXPERT + member) * 2 + heading) * CAP + within
    anchor = ((heading * PIPE + section) * N_EXPERT + member) * TOK_DEV + entry // TOP
    length = PIPE * N_EXPERT * 2 * CAP
    owner = jnp.full((EXPERTS, length), 2 * PIPE * TOKENS, jnp.int32).at[groups, place].set(anchor)
    width = hidden.shape[-1]
    table = jnp.concatenate([hidden.reshape(-1, width), jnp.zeros((1, width), jnp.bfloat16)], axis=0)

    def expert_rows(pieces):
        owned, upper, lower = pieces
        inner = jnp.dot(table[owned], upper, preferred_element_type=jnp.float32)
        active = jax.nn.silu(inner).astype(jnp.bfloat16)
        return jnp.dot(active, lower, preferred_element_type=jnp.float32).astype(jnp.bfloat16)
    produced = lax.map(expert_rows, (owner, w_up, w_down))

    def combine(pieces):
        chosen, spots, weights = pieces
        rows = produced[chosen, spots].astype(jnp.float32)
        rows = rows.reshape(N_EXPERT * TOK_DEV, TOP, width)
        return jnp.einsum('tk,tkc->tc', weights, rows)
    mixed = lax.map(combine, (groups.reshape(2 * PIPE, N_EXPERT, TOK_DEV * TOP), place.reshape(2 * PIPE, N_EXPERT, TOK_DEV * TOP), gates.reshape(2 * PIPE, TOKENS, TOP)))
    result = arrived + mixed.reshape(arrived.shape)
    return result.astype(jnp.bfloat16)
```

```python
import jax
import jax.numpy as jnp
from jax import lax
from jax.sharding import PartitionSpec as P

norm_eps = 1e-06
route_scale = 2.5
few = 8


def shifted(x, axis, by):
    size = lax.axis_size(axis)
    return lax.ppermute(x, axis, [(i, (i + by) % size) for i in range(size)])


def summed(own, sent, axis):
    for by in range(1, lax.axis_size(axis)):
        own = own + shifted(sent, axis, by).astype(own.dtype)
    return own


def swapped(blocks, axis, sign):
    size = lax.axis_size(axis)
    if size > few:
        return lax.all_to_all(blocks, axis, split_axis=0, concat_axis=0, tiled=True)
    moved = {by: shifted(blocks[by], axis, sign * by) for by in sorted(range(1, size), key=lambda b: abs(2 * b - size))}
    return jnp.stack([blocks[0]] + [moved[by] for by in range(1, size)])


def shards(stream, expert_ids, norm_gain, router, w_up, w_down):
    ahead = shifted(stream[0], "pipe", 1)
    behind = shifted(stream[1], "pipe", -1)
    tok_rows, quarter = stream.shape[2:]
    chosen = expert_ids[:, 0]
    fanout = chosen.shape[2]
    experts = router.shape[2]
    size = lax.axis_size("expert")
    width = float(quarter * lax.axis_size("tensor"))
    capacity = 3 * tok_rows * fanout // (2 * experts)
    bf16, f32 = jnp.bfloat16, jnp.float32

    flat = chosen.reshape(2, tok_rows * fanout)
    order = jnp.arange(tok_rows * fanout)
    same = (flat[:, :, None] == flat[:, None, :]) & (order[None, :] < order[:, None])
    within = jnp.sum(same.astype(jnp.int32), axis=-1)
    block = flat if size > few else (flat - lax.axis_index("expert")) % size
    target = block * (2 * capacity) + jnp.arange(2)[:, None] * capacity + within
    slots = jnp.arange(experts * 2 * capacity)
    placed = target.reshape(2 * tok_rows, fanout)
    spread = (slots[:, None, None] == placed[None]).any(axis=-1).astype(bf16)
    fetch = (placed.T.reshape(-1, 1) == slots[None]).astype(bf16)

    rows = jnp.concatenate([ahead, behind], axis=0).reshape(2 * tok_rows, quarter)
    outgoing = jnp.dot(spread, rows, preferred_element_type=f32).astype(bf16)
    received = swapped(outgoing.reshape(experts, 2 * capacity, quarter), "expert", 1)
    received = received.reshape(-1, quarter).astype(f32)

    arrived = rows.astype(f32)
    part = jnp.dot(arrived * norm_gain, router[0], precision=lax.Precision.HIGHEST)
    square = jnp.sum(arrived * arrived, axis=-1, keepdims=True)
    both = jnp.concatenate([part, square], axis=1)
    both = summed(both, both, "tensor")
    logits = both[:, :experts] * lax.rsqrt(both[:, experts:] / width + norm_eps)
    picks = chosen.reshape(2 * tok_rows, fanout, 1) == jnp.arange(experts)
    scores = jax.nn.sigmoid(jnp.sum(jnp.where(picks, logits[:, None], 0.0), axis=-1))
    gates = route_scale * scores / jnp.sum(scores, axis=-1, keepdims=True)

    hidden = (received * norm_gain).astype(bf16)
    squares = jnp.sum(received * received, axis=-1, keepdims=True)
    squares = summed(squares, squares, "tensor")
    inverse = lax.rsqrt(squares / width + norm_eps)
    inner = jnp.dot(hidden, w_up[0], preferred_element_type=f32)
    inner = summed(inner, inner.astype(bf16), "tensor") * inverse
    active = jax.nn.silu(inner).astype(bf16)
    produced = jnp.dot(active, w_down[0], preferred_element_type=f32).astype(bf16)
    answers = swapped(produced.reshape(experts, 2 * capacity, quarter), "expert", -1)

    answers = answers.reshape(-1, quarter)
    gathered = jnp.dot(fetch, answers, preferred_element_type=f32).reshape(fanout, 2 * tok_rows, quarter)
    mixed = jnp.sum(gates.T[..., None] * gathered, axis=0)
    result = (arrived + mixed).astype(bf16)
    return result.reshape(stream.shape)


def solution(mesh):
    return jax.shard_map(
        shards,
        mesh=mesh,
        in_specs=(
            P(None, "pipe", "expert", "tensor"),
            P(None, "pipe", "expert", None),
            P("pipe", "tensor"),
            P("pipe", "tensor", None),
            P("expert", "tensor", None),
            P("expert", None, "tensor"),
        ),
        out_specs=P(None, "pipe", "expert", "tensor"),
        check_vma=False,
    )
```

```python
import jax
import jax.numpy as jnp
from jax import lax
from jax.experimental import pallas as pl
from jax.experimental.pallas import tpu as pltpu
from jax.sharding import PartitionSpec as P

norm_eps = 1e-06
route_scale = 2.5
few = 8


def shifted(x, axis, by):
    size = lax.axis_size(axis)
    return lax.ppermute(x, axis, [(i, (i + by) % size) for i in range(size)])


def summed(own, sent, axis):
    for by in range(1, lax.axis_size(axis)):
        own = own + shifted(sent, axis, by).astype(own.dtype)
    return own


def to_vmem(weights):
    def body(source, target, done):
        copy = pltpu.make_async_copy(source, target, done)
        copy.start()
        copy.wait()

    return pl.pallas_call(
        body,
        in_specs=[pl.BlockSpec(memory_space=pl.ANY)],
        out_specs=pl.BlockSpec(memory_space=pltpu.VMEM),
        out_shape=pltpu.VMEM(weights.shape, weights.dtype),
        scratch_shapes=[pltpu.SemaphoreType.DMA],
        compiler_params=pltpu.CompilerParams(vmem_limit_bytes=1 << 20),
        name="to_vmem",
    )(weights)


def shards(stream, expert_ids, norm_gain, router, w_up, w_down):
    ahead = shifted(stream[0], "pipe", 1)
    behind = shifted(stream[1], "pipe", -1)
    tok_rows, quarter = stream.shape[2:]
    chosen = expert_ids[:, 0]
    fanout = chosen.shape[2]
    experts = router.shape[2]
    size = lax.axis_size("expert")
    width = float(quarter * lax.axis_size("tensor"))
    capacity = 3 * tok_rows * fanout // (2 * experts)
    bf16, f32 = jnp.bfloat16, jnp.float32

    flat = chosen.reshape(2, tok_rows * fanout)
    order = jnp.arange(tok_rows * fanout)
    same = (flat[:, :, None] == flat[:, None, :]) & (order[None, :] < order[:, None])
    within = jnp.sum(same.astype(jnp.int32), axis=-1)
    block = flat if size > few else (flat - lax.axis_index("expert")) % size
    target = block * (2 * capacity) + jnp.arange(2)[:, None] * capacity + within
    slots = jnp.arange(experts * 2 * capacity)
    placed = target.reshape(2 * tok_rows, fanout)
    spread = (slots[:, None, None] == placed[None]).any(axis=-1).astype(bf16)
    fetch = (placed.T.reshape(-1, 1) == slots[None]).astype(bf16)

    rows = jnp.concatenate([ahead, behind], axis=0).reshape(2 * tok_rows, quarter)
    span = 2 * capacity

    def picked(blocks, source):
        out = jnp.dot(jnp.concatenate([spread[by * span : by * span + span] for by in blocks]), source, preferred_element_type=f32)
        return out.astype(bf16).reshape(len(blocks), span, quarter)

    half = size // 2
    groups = [[0, half], [by for by in range(1, size) if by != half]] if size <= few else [list(range(size))]
    upper, lower = w_up[0], w_down[0]
    first = picked(groups[0], rows)
    if size > few:
        blocks = lax.all_to_all(first, "expert", split_axis=0, concat_axis=0, tiled=True)
    else:
        blocks = {0: first[0]}
        blocks[half] = shifted(first[1], "expert", half)
        upper, rows, first = lax.optimization_barrier((upper, rows, first))
        upper = to_vmem(upper)

    arrived = rows.astype(f32)
    scaled = arrived * norm_gain
    part = jnp.dot(scaled, router[0], precision=lax.Precision.HIGHEST)
    square = jnp.sum(arrived * arrived, axis=-1, keepdims=True)
    both = jnp.concatenate([part, square], axis=1)
    both = summed(both, both, "tensor")
    home_inverse = lax.rsqrt(both[:, experts:] / width + norm_eps)
    if size <= few:
        second = picked(groups[1], (scaled * home_inverse).astype(bf16))
        for place, by in enumerate(groups[1]):
            blocks[by] = shifted(second[place], "expert", by)
    logits = both[:, :experts] * home_inverse
    picks = chosen.reshape(2 * tok_rows, fanout, 1) == jnp.arange(experts)
    scores = jax.nn.sigmoid(jnp.sum(jnp.where(picks, logits[:, None], 0.0), axis=-1))
    gates = route_scale * scores / jnp.sum(scores, axis=-1, keepdims=True)

    answers = {}
    for tag, group in zip("ab", groups):
        raw = jnp.concatenate([blocks[by] for by in group])
        if tag == "a":
            wide = raw.astype(f32)
            squares = jnp.sum(wide * wide, axis=-1, keepdims=True)
            squares = summed(squares, squares, "tensor")
            inverse = lax.rsqrt(squares / width + norm_eps)
        hidden = (wide * norm_gain).astype(bf16) if tag == "a" else raw
        inner = jnp.dot(hidden, upper, preferred_element_type=f32)
        sent = inner.astype(bf16)
        inner = summed(inner, sent, "tensor")
        inner = inner * inverse if tag == "a" else inner
        active = jax.nn.silu(inner).astype(bf16)
        produced = jnp.dot(active, lower, preferred_element_type=f32).astype(bf16)
        produced = produced.reshape(len(group), 2 * capacity, quarter)
        for place, by in enumerate(group):
            if size > few or not by:
                answers[by] = produced[place]
                continue
            answers[by] = shifted(produced[place], "expert", -by)
    answers = jnp.stack([answers[by] for by in range(size)])
    if size > few:
        answers = lax.all_to_all(answers, "expert", split_axis=0, concat_axis=0, tiled=True)

    answers = answers.reshape(-1, quarter)
    gathered = jnp.dot(fetch, answers, preferred_element_type=f32).reshape(fanout, 2 * tok_rows, quarter)
    mixed = jnp.sum(gates.T[..., None] * gathered, axis=0)
    result = (arrived + mixed).astype(bf16)
    return result.reshape(stream.shape)


def solution(mesh):
    return jax.shard_map(
        shards,
        mesh=mesh,
        in_specs=(
            P(None, "pipe", "expert", "tensor"),
            P(None, "pipe", "expert", None),
            P("pipe", "tensor"),
            P("pipe", "tensor", None),
            P("expert", "tensor", None),
            P("expert", None, "tensor"),
        ),
        out_specs=P(None, "pipe", "expert", "tensor"),
        check_vma=False,
    )
```
